32 devices in a mesh: ctx: 8 (over y, x, core), rec: 4 (over z).
Axes of the slice: x: 2, y: 2, z: 4, core: 2. Of those that a mesh axis runs over, the one named last changes fastest.
Arguments:
- queries: bfloat16 [4, 1024, 4096], P('rec', 'ctx'), may hold values from -6 to 6
- out_grads: bfloat16 [4, 1024, 4096], P('rec', 'ctx'), may hold values from -6 to 6
- log_sums: float32 [4, 32, 1024], P('rec', None, 'ctx'), may hold values from 1.5 to 4
- deltas: float32 [4, 32, 1024], P('rec', None, 'ctx'), may hold values from -6 to 6
- keys: bfloat16 [1024, 256], P('ctx'), may hold values from -6 to 6
- values: bfloat16 [1024, 256], P('ctx'), may hold values from -0.5 to 0.5
- doc_ids: int32 [4, 8], P('rec'), may hold values from 0 to 3, never falling along the last dimension, each value on 1 to 4 neighbouring positions
Outputs:
- query_grads: bfloat16 [4, 1024, 4096], P('rec', 'ctx')
- key_grads: bfloat16 [1024, 256], P(('ctx', 'rec'))
- value_grads: bfloat16 [1024, 256], P(('ctx', 'rec'))
The draws below stay inside these ranges and needn't reach their ends.
Inputs may be any that keep to these rules, and one draw needn't show every extreme that they name: `doc_ids`: in each row the numbers never fall, start at 0, each document spans 1 to 4 blocks and some document spans exactly 4 blocks.
All inputs are finite; a program needn't handle non-finite values.
Results may differ from the reference program's by a relative error of at most 0.0062.
Values may be sent and summed in bfloat16 or wider, within the bound.
A program may use at most 64 MiB of HBM per device.

```python
import math
import jax
import jax.numpy as jnp
import numpy as np
from jax import lax

QH = 32
KVH = 2
HD = 128
TOK = 128
MAXSPAN = 4
NBLK = 8
REC = 4
TOKENS = 1024


def block_scale(key, dims, pieces, low, top_value):
    factor_of, own = 1.0, jax.random.fold_in(key, 6)
    for position, shards_of in pieces:
        heights = jnp.exp(jax.random.uniform(jax.random.fold_in(own, position), (shards_of,), jnp.float32, low / len(pieces), top_value / len(pieces)))
        factor_of = factor_of * jnp.repeat(heights, dims[position] // shards_of).reshape([-1 if axis == position else 1 for axis in range(len(dims))])
    return factor_of


def split_up(amount, total, limit, skew):
    loads = [(1 << 20) // math.isqrt(rank ** skew) + 1 for rank in range(2, amount + 1)]
    spare, holding = total - limit - (amount - 1), [1] * (amount - 1)
    while spare > 0:
        free = [i for i in range(amount - 1) if holding[i] < limit]
        pool, budget = sum([loads[i] for i in free]), spare
        for i in free:
            addition = min(limit - holding[i], max(1, budget * loads[i] // pool), spare)
            holding[i] = holding[i] + addition
            spare = spare - addition
    return np.array([limit] + holding)


def ragged_sizes(stream_key, count, total, bound, slope):
    if count == 2:
        one = jax.random.randint(stream_key, (), max(1, total - bound), min(bound, total - 1) + 1)
        return jnp.stack([one, total - one])
    lengths = jnp.asarray(split_up(count, total, bound, slope), jnp.int32)
    couples = (count - 1) // 2
    donor, taker = lengths[1:1 + 2 * couples:2], lengths[2:2 + 2 * couples:2]
    slack = jnp.minimum(donor - 1, bound - taker)
    shifted = jax.random.randint(jax.random.fold_in(stream_key, 1), (couples,), 0, 1 << 20) % (slack + 1)
    lengths = lengths.at[1:1 + 2 * couples:2].set(donor - shifted).at[2:2 + 2 * couples:2].set(taker + shifted)
    return lengths[jax.random.permutation(jax.random.fold_in(stream_key, 2), count)]


def normal_values(key, extent, scale, most, pieces=(), kind=jnp.bfloat16):
    result = jax.random.normal(key, extent, jnp.float32) * scale
    if len(pieces) > 0:
        result = block_scale(key, extent, pieces, -0.22, 0.18) * result
    return jnp.clip(result, min=-most, max=most).astype(kind)


def setup_inputs(seed: int = 0) -> dict:
    arg_keys = jax.random.split(jax.random.key(seed), 8)
    queries = normal_values(arg_keys[0], (REC, TOKENS, QH * HD), 1.0, 6.0, ((0, 4), (1, 8)))
    out_grads = normal_values(arg_keys[1], (REC, TOKENS, QH * HD), 1.0, 6.0, ((0, 4), (1, 8)))
    log_sums = jnp.clip(1.5 + 2.5 * jax.random.uniform(arg_keys[2], (REC, QH, TOKENS), jnp.float32) ** block_scale(arg_keys[2], (REC, QH, TOKENS), ((0, 4), (2, 8)), -0.2, 0.2), 1.5, 4.0)
    deltas = normal_values(arg_keys[3], (REC, QH, TOKENS), 1.0, 6.0, ((0, 4), (2, 8)), jnp.float32)
    keys = normal_values(arg_keys[4], (TOKENS, KVH * HD), 1.0, 6.0, ((0, 8),))
    values = normal_values(arg_keys[5], (TOKENS, KVH * HD), HD ** -0.5, 0.5, ((0, 8),))
    doc_ids = jax.vmap(lambda own: jnp.searchsorted(jnp.cumsum(ragged_sizes(own, NBLK // 2, NBLK, MAXSPAN, 1)), jnp.arange(NBLK), side="right"))(jax.random.split(arg_keys[6], REC)).reshape((REC, NBLK)).astype(jnp.int32)
    return {"queries": queries, "out_grads": out_grads, "log_sums": log_sums, "deltas": deltas, "keys": keys, "values": values, "doc_ids": doc_ids}


def tile_terms(query_block, grad_block, sums_block, delta_block, key_block, value_block, query_index, key_index):
    rows = query_block.shape[0]
    key_heads = key_block.shape[1] // HD
    group = query_block.shape[1] // (key_heads * HD)
    scale = HD ** -0.5
    query_heads = query_block.astype(jnp.float32).reshape(rows, key_heads, group, HD)
    grad_heads = grad_block.astype(jnp.float32).reshape(rows, key_heads, group, HD)
    key_split = key_block.astype(jnp.float32).reshape(rows, key_heads, HD)
    value_split = value_block.astype(jnp.float32).reshape(rows, key_heads, HD)
    sums_heads = sums_block.reshape(key_heads, group, rows)
    delta_heads = delta_block.reshape(key_heads, group, rows)
    positions = jnp.arange(rows, dtype=jnp.int32)
    query_pos = query_index * rows + positions
    key_pos = key_index * rows + positions
    causal = key_pos[None, :] <= query_pos[:, None]
    scores = jnp.einsum("qkgd,skd->kgqs", query_heads, key_split) * scale
    probs = jnp.where(causal, jnp.exp(scores - sums_heads[..., None]), 0.0)
    dprobs = jnp.einsum("qkgd,skd->kgqs", grad_heads, value_split)
    dscores = probs * (dprobs - delta_heads[..., None])
    probs_b = probs.astype(jnp.bfloat16).astype(jnp.float32)
    dscores_b = dscores.astype(jnp.bfloat16).astype(jnp.float32)
    value_grad = jnp.einsum("kgqs,qkgd->skd", probs_b, grad_heads).reshape(rows, key_heads * HD)
    key_grad = jnp.einsum("kgqs,qkgd->skd", dscores_b, query_heads).reshape(rows, key_heads * HD) * scale
    query_grad = jnp.einsum("kgqs,skd->qkgd", dscores_b, key_split).reshape(rows, -1) * scale
    return query_grad, key_grad, value_grad


def reference(queries, out_grads, log_sums, deltas, keys, values, doc_ids):
    rows = TOK
    span = MAXSPAN
    blocks = NBLK
    width = keys.shape[1]
    qwidth = queries.shape[2]
    pad_rows = (span - 1) * rows
    keys_pad = jnp.concatenate([jnp.zeros((pad_rows, width), keys.dtype), keys], axis=0)
    values_pad = jnp.concatenate([jnp.zeros((pad_rows, width), values.dtype), values], axis=0)
    key_total = jnp.zeros((pad_rows + TOKENS, width), jnp.float32)
    value_total = jnp.zeros((pad_rows + TOKENS, width), jnp.float32)
    order = jnp.arange(blocks, dtype=jnp.int32)
    results = []
    for recur in range(REC):
        ids = doc_ids[recur]
        first = jnp.min(jnp.where(ids[:, None] == ids[None, :], order[None, :], blocks), axis=1).astype(jnp.int32)
        query_all = queries[recur]
        grad_all = out_grads[recur]
        sums_all = log_sums[recur]
        delta_all = deltas[recur]

        def per_block(carry, index):
            key_acc, value_acc = carry
            start = (index * rows).astype(jnp.int32)
            query_block = lax.dynamic_slice_in_dim(query_all, start, rows, 0)
            grad_block = lax.dynamic_slice_in_dim(grad_all, start, rows, 0)
            sums_block = lax.dynamic_slice_in_dim(sums_all, start, rows, 1)
            delta_block = lax.dynamic_slice_in_dim(delta_all, start, rows, 1)
            query_grad = jnp.zeros((rows, qwidth), jnp.float32)
            for back in range(span):
                other = index - back
                kstart = ((other + span - 1) * rows).astype(jnp.int32)
                key_block = lax.dynamic_slice_in_dim(keys_pad, kstart, rows, 0)
                value_block = lax.dynamic_slice_in_dim(values_pad, kstart, rows, 0)
                active = other >= first[index]

                def compute():
                    return tile_terms(query_block, grad_block, sums_block, delta_block, key_block, value_block, index, other)

                def nothing():
                    return (jnp.zeros((rows, qwidth), jnp.float32), jnp.zeros((rows, width), jnp.float32), jnp.zeros((rows, width), jnp.float32))

                terms = lax.cond(active, compute, nothing)
                query_grad = query_grad + terms[0]
                key_acc = lax.dynamic_update_slice_in_dim(key_acc, lax.dynamic_slice_in_dim(key_acc, kstart, rows, 0) + terms[1], kstart, 0)
                value_acc = lax.dynamic_update_slice_in_dim(value_acc, lax.dynamic_slice_in_dim(value_acc, kstart, rows, 0) + terms[2], kstart, 0)
            return (key_acc, value_acc), query_grad.astype(jnp.bfloat16)

        (key_total, value_total), grads = lax.scan(per_block, (key_total, value_total), order)
        results.append(grads.reshape(TOKENS, qwidth))
    query_grads = jnp.stack(results, axis=0)
    return query_grads, key_total[pad_rows:].astype(jnp.bfloat16), value_total[pad_rows:].astype(jnp.bfloat16)
```

```python
import math

import jax
import jax.numpy as jnp
from jax import lax
from jax.experimental import pallas as pl
from jax.experimental.pallas import tpu as pltpu
from jax.sharding import PartitionSpec as P

HD = 128
MAXSPAN = 4
HEADS = 16
BACK = MAXSPAN - 1
MESH = pl.DeviceIdType.MESH
FAR = 1e30
PIECES = 4


def kernel(
    q_hbm, g_hbm, sums_hbm, delta_hbm, k_hbm, v_hbm, ids_hbm,
    dq_ref, dk_ref, dv_ref,
    q_buf, g_buf, sums_ref, delta_ref, ids_ref, kv, key_t, ds_buf, acc, part, mate, side_land, back_land,
    direct_land, total, r_send, r_land,
    load_sem, own_sem, small_sem, hop_sem, near_sem, far_sem, pass_sem, mate_sem, side_sem, back_sem,
    direct_sem, rec_sem,
):
    peers = lax.axis_size("ctx")
    recs = lax.axis_size("rec")
    mine = lax.axis_index("ctx")
    rec = lax.axis_index("rec")
    rows = q_buf.shape[0]
    key_heads = kv.shape[0]
    group = q_buf.shape[1] // (key_heads * HD)
    chunks = group // HEADS
    wide = HEADS * HD
    scale = HD ** (-0.5)
    fold = scale * math.log2(math.e)
    share = rows // recs
    last = key_heads - 1
    odd = lax.rem(mine, 2)
    even = 1 - odd
    partner = mine + even - odd
    first_k = 1 + 2 * odd
    side_k = 3 - 2 * odd

    def slot(k):
        if isinstance(k, int):
            return pl.ds(k * rows, rows)
        return pl.ds(pl.multiple_of(k * rows, rows), rows)

    def own_copy(g, which):
        source = (k_hbm, v_hbm)[which]
        return pltpu.make_async_copy(
            source.at[:, pl.ds(g * HD, HD)], kv.at[g, which, pl.ds(0, rows), :], own_sem.at[g, which]
        )

    def lanes(g, c):
        return pl.ds(pl.multiple_of((g * chunks + c) * wide, wide), wide)

    def load(g, c, which):
        source, target = ((q_hbm, q_buf), (g_hbm, g_buf))[which]
        return pltpu.make_async_copy(
            source.at[0, :, lanes(g, c)], target.at[:, lanes(g, c)], load_sem.at[g, c, which]
        )

    def remote(source, target, sems, device):
        return pltpu.make_async_remote_copy(
            src_ref=source, dst_ref=target, send_sem=sems.at[0], recv_sem=sems.at[1],
            device_id=device, device_id_type=MESH,
        )

    def hop(g):
        return remote(kv.at[g, :, slot(0), :], kv.at[g, :, slot(2), :], hop_sem.at[g], {"ctx": lax.rem(mine + 2, peers)})

    def near(g):
        return remote(kv.at[g, :, slot(0), :], kv.at[g, :, slot(1), :], near_sem.at[g], {"ctx": partner})

    def far(g):
        return remote(kv.at[g, :, slot(0), :], kv.at[g, :, slot(3), :], far_sem.at[g], {"ctx": lax.rem(mine + 3, peers)})

    def hand(g):
        return remote(kv.at[g, :, slot(2), :], kv.at[g, :, slot(side_k), :], pass_sem.at[g], {"ctx": partner})

    def mate_copy(g):
        return remote(part.at[g, first_k - 1], mate.at[g], mate_sem.at[g], {"ctx": partner})

    def side_copy(g):
        return remote(part.at[g, side_k - 1], side_land.at[g], side_sem.at[g], {"ctx": lax.rem(mine - side_k + peers, peers)})

    def back_copy(g):
        return remote(part.at[g, 1], back_land.at[g], back_sem.at[g], {"ctx": lax.rem(mine - 2 + peers, peers)})

    def shares(ref, target):
        return ref.at[:, pl.ds(pl.multiple_of(target * share, share), share), :]

    def direct_copy(j):
        target = lax.rem(rec + j, recs)
        return remote(
            shares(part.at[last, 1], target), direct_land.at[j], direct_sem.at[j],
            {"ctx": lax.rem(mine - 2 + peers, peers), "rec": target},
        )

    def rec_copy(g, j):
        target = lax.rem(rec + j, recs)
        return remote(shares(r_send.at[g], target), r_land.at[g, j - 1], rec_sem.at[g, j - 1], {"rec": target})

    for g in range(key_heads):
        for which in range(2):
            own_copy(g, which).start()
    small = [
        pltpu.make_async_copy(source, target, small_sem.at[i])
        for i, (source, target) in enumerate(
            ((sums_hbm, sums_ref), (delta_hbm, delta_ref), (ids_hbm, ids_ref))
        )
    ]
    for copy in small:
        copy.start()
    for g in range(key_heads):
        for c in range(chunks):
            for which in range(2):
                load(g, c, which).start()

    barrier = pltpu.get_barrier_semaphore()
    third = lax.rem(mine + 3 * odd - 3 * even + peers, peers)
    for other in (partner, lax.rem(mine + 2, peers), lax.rem(mine - 2 + peers, peers), third):
        pl.semaphore_signal(barrier, inc=1, device_id={"ctx": other}, device_id_type=MESH)
    for j in range(1, recs):
        pl.semaphore_signal(
            barrier, inc=1, device_id={"rec": lax.rem(rec + j, recs)}, device_id_type=MESH
        )
    for k in range(1, MAXSPAN):
        @pl.when(mine < k)
        def _():
            kv[:, :, pl.ds(k * rows, rows), :] = jnp.zeros((key_heads, 2, rows, HD), kv.dtype)

    @pl.when(mine < 2)
    def _():
        mate[...] = jnp.zeros_like(mate)

    @pl.when(mine + 2 >= peers)
    def _():
        back_land[...] = jnp.zeros_like(back_land)
        direct_land[...] = jnp.zeros_like(direct_land)

    @pl.when((odd == 1) & (mine + 3 >= peers))
    def _():
        side_land[...] = jnp.zeros_like(side_land)

    acc[...] = jnp.zeros_like(acc)
    pl.semaphore_wait(barrier, 4 + recs - 1)

    for g in range(key_heads):
        for which in range(2):
            own_copy(g, which).wait()

        @pl.when(mine + 2 < peers)
        def _():
            hop(g).start()

        @pl.when(even == 1)
        def _():
            near(g).start()

        @pl.when((odd == 1) & (mine + 3 < peers))
        def _():
            far(g).start()

    for copy in small:
        copy.wait()
    here = ids_ref[0, mine]

    def away(k):
        if isinstance(k, int) and k == 0:
            return jnp.float32(0.0)
        same = (ids_ref[0, jnp.maximum(mine - k, 0)] == here) & (mine >= k)
        return jnp.where(same, 0.0, FAR).astype(jnp.float32)

    def heads_down(ref, g, c):
        first = (g * chunks + c) * HEADS
        return jnp.concatenate(
            [ref[:, pl.ds(pl.multiple_of((first + i) * HD, HD), HD)] for i in range(HEADS)], axis=0
        )

    def heads_along(ref, g, c):
        first = (g * chunks + c) * HEADS
        return jnp.concatenate([ref[0, pl.ds(first + i, 1), :] for i in range(HEADS)], axis=1)

    inner = (((1,), (1,)), ((), ()))

    def sweep(g, k):
        at = slot(k)
        own = isinstance(k, int) and k == 0
        shift = away(k)

        @pl.loop(0, chunks)
        def _(c):
            if own:
                for which in range(2):
                    load(g, c, which).wait()
            query = heads_down(q_buf, g, c)
            grad = heads_down(g_buf, g, c)
            sums = heads_along(sums_ref, g, c) * math.log2(math.e) + shift
            delta = heads_along(delta_ref, g, c)
            scores = lax.dot_general(
                kv[g, 0, at, :], query, inner, preferred_element_type=jnp.float32
            )
            dprobs = lax.dot_general(
                kv[g, 1, at, :], grad, inner, preferred_element_type=jnp.float32
            )
            probs = jnp.exp2(scores * fold - sums)
            if own:
                u = lax.broadcasted_iota(jnp.int32, (rows, wide), 0)
                t = lax.broadcasted_iota(jnp.int32, (rows, wide), 1) & (rows - 1)
                probs = jnp.where(u <= t, probs, 0.0)
            ds = (probs * (dprobs - delta)).astype(jnp.bfloat16)
            probs = probs.astype(jnp.bfloat16)
            ds_buf[at, lanes(g, c)] = ds
            acc[g, 0, at, :] += jnp.dot(ds, query, preferred_element_type=jnp.float32)
            acc[g, 1, at, :] += jnp.dot(probs, grad, preferred_element_type=jnp.float32)

        key_t[g, :, slot(k)] = kv[g, 0, at, :].T

    def query_side(g):
        @pl.loop(0, chunks)
        def _(c):
            dq = jnp.dot(
                key_t[g], ds_buf[:, lanes(g, c)], preferred_element_type=jnp.float32
            ) * scale
            for i in range(HEADS):
                at = pl.ds(pl.multiple_of(((g * chunks + c) * HEADS + i) * HD, HD), HD)
                dq_ref[0, :, at] = dq[:, i * rows:(i + 1) * rows].T.astype(dq_ref.dtype)

    def keep(g, k):
        part[g, k - 1] = acc[g, :, slot(k), :].astype(part.dtype)

    def arrive(g):
        @pl.when(mine >= 2)
        def _():
            hop(g).wait_recv()
            hand(g).start()

    def combine(g):
        @pl.when(mine >= 2)
        def _():
            mate_copy(g).wait_recv()
        part[g, 1] = (acc[g, :, slot(2), :] + mate[g].astype(jnp.float32)).astype(part.dtype)

        @pl.when(mine >= 2)
        def _():
            if g == last:
                for j in range(recs):
                    direct_copy(j).start()
            else:
                back_copy(g).start()

    def send_mate(g):
        keep(g, first_k)

        @pl.when(mine >= 2)
        def _():
            mate_copy(g).start()

    def send_side(g):
        keep(g, side_k)

        @pl.when(mine >= side_k)
        def _():
            side_copy(g).start()

    def wait_far(g):
        @pl.when((even == 1) & (mine >= 3))
        def _():
            far(g).wait_recv()

    def wait_near(g):
        @pl.when(odd == 1)
        def _():
            near(g).wait_recv()

    def wait_hand(g):
        @pl.when(mine >= 2)
        def _():
            hand(g).wait_recv()

    def across(g):
        whole = acc[g, :, 0:rows, :]

        @pl.when((even == 1) | (mine + 3 < peers))
        def _():
            side_copy(g).wait_recv()
        whole = whole + side_land[g].astype(jnp.float32)
        if g != last:
            @pl.when(mine + 2 < peers)
            def _():
                back_copy(g).wait_recv()
            whole = whole + back_land[g].astype(jnp.float32)
        total[g] = whole
        r_send[g] = whole.astype(r_send.dtype)
        for j in range(1, recs):
            rec_copy(g, j).start()

    def close(g):
        whole = total[g, :, pl.ds(pl.multiple_of(rec * share, share), share), :]
        for j in range(1, recs):
            rec_copy(g, j).wait_recv()
            whole = whole + r_land[g, j - 1].astype(jnp.float32)
        if g == last:
            @pl.when(mine + 2 < peers)
            def _():
                for j in range(recs):
                    direct_copy(j).wait_recv()
            for j in range(recs):
                whole = whole + direct_land[j].astype(jnp.float32)
        dk_ref[:, g * HD:(g + 1) * HD] = (whole[0] * scale).astype(dk_ref.dtype)
        dv_ref[:, g * HD:(g + 1) * HD] = whole[1].astype(dv_ref.dtype)

    for g in range(key_heads):
        sweep(g, 0)
    arrive(0)
    for g in range(key_heads):
        if g == 0:
            wait_near(g)
            sweep(g, 2 - odd)
            if g < last:
                arrive(g + 1)
            wait_far(g)
            sweep(g, 3 - odd)
            send_side(g)
            wait_hand(g)
            sweep(g, first_k)
            send_mate(g)
        else:
            wait_near(g)
            wait_hand(g)
            sweep(g, first_k)
            send_mate(g)
            combine(g - 1)
            if g < last:
                arrive(g + 1)
            wait_far(g)
            sweep(g, side_k)
            send_side(g)
            sweep(g, 2)
    combine(last)
    for g in range(last):
        across(g)
        query_side(g)
    across(last)
    query_side(last)
    for g in range(key_heads):
        close(g)
    for g in range(key_heads):
        @pl.when(mine + 2 < peers)
        def _():
            hop(g).wait_send()

        @pl.when(even == 1)
        def _():
            near(g).wait_send()

        @pl.when((odd == 1) & (mine + 3 < peers))
        def _():
            far(g).wait_send()

        @pl.when(mine >= 2)
        def _():
            hand(g).wait_send()
            mate_copy(g).wait_send()
            if g == last:
                for j in range(recs):
                    direct_copy(j).wait_send()
            else:
                back_copy(g).wait_send()

        @pl.when(mine >= side_k)
        def _():
            side_copy(g).wait_send()
        for j in range(1, recs):
            rec_copy(g, j).wait_send()


def finish(dq_in, dk_in, dv_in, dq_out, dk_out, dv_out, out):
    depth = dq_in.shape[1] // PIECES
    pairs = [
        (dq_in.at[0, pl.ds(i * depth, depth), :], dq_out.at[0, pl.ds(i * depth, depth), :])
        for i in range(PIECES)
    ] + [(dk_in, dk_out), (dv_in, dv_out)]
    outs = [pltpu.make_async_copy(p[0], p[1], out.at[i]) for i, p in enumerate(pairs)]
    for copy in outs:
        copy.start()
    for copy in outs:
        copy.wait()


def per_device(queries, out_grads, log_sums, deltas, keys, values, doc_ids):
    recs = lax.axis_size("rec")
    rows, width = queries.shape[1:]
    key_heads = keys.shape[1] // HD
    chunks = width // (key_heads * HD * HEADS)
    span = MAXSPAN * rows
    half = jnp.bfloat16
    dma = pltpu.SemaphoreType.DMA
    far_off = pl.BlockSpec(memory_space=pltpu.HBM)
    vmem = pl.BlockSpec(memory_space=pltpu.VMEM)
    small = (rows // recs, keys.shape[1])
    shapes = (
        jax.ShapeDtypeStruct(queries.shape, half),
        jax.ShapeDtypeStruct(small, half),
        jax.ShapeDtypeStruct(small, half),
    )
    pair = (key_heads, 2, rows, HD)
    grads = pl.pallas_call(
        kernel,
        out_shape=shapes,
        in_specs=[far_off] * 7,
        out_specs=(vmem, vmem, vmem),
        scratch_shapes=[
            pltpu.VMEM((rows, width), half),
            pltpu.VMEM((rows, width), half),
            pltpu.VMEM(log_sums.shape, jnp.float32),
            pltpu.VMEM(deltas.shape, jnp.float32),
            pltpu.SMEM(doc_ids.shape, jnp.int32),
            pltpu.VMEM((key_heads, 2, span, HD), half),
            pltpu.VMEM((key_heads, HD, span), half),
            pltpu.VMEM((span, width), half),
            pltpu.VMEM((key_heads, 2, span, HD), jnp.float32),
            pltpu.VMEM((key_heads, BACK, 2, rows, HD), half),
            pltpu.VMEM(pair, half),
            pltpu.VMEM(pair, half),
            pltpu.VMEM(pair, half),
            pltpu.VMEM((recs, 2, rows // recs, HD), half),
            pltpu.VMEM(pair, jnp.float32),
            pltpu.VMEM(pair, half),
            pltpu.VMEM((key_heads, max(recs - 1, 1), 2, rows // recs, HD), half),
            dma((key_heads, chunks, 2)),
            dma((key_heads, 2)),
            dma((3,)),
            dma((key_heads, 2)),
            dma((key_heads, 2)),
            dma((key_heads, 2)),
            dma((key_heads, 2)),
            dma((key_heads, 2)),
            dma((key_heads, 2)),
            dma((key_heads, 2)),
            dma((recs, 2)),
            dma((key_heads, max(recs - 1, 1), 2)),
        ],
        compiler_params=pltpu.CompilerParams(
            collective_id=0, has_side_effects=True, vmem_limit_bytes=40 * 2**20
        ),
    )(*[
        pltpu.with_memory_space_constraint(x, pltpu.HBM)
        for x in (queries, out_grads, log_sums, deltas, keys, values, doc_ids)
    ])
    return pl.pallas_call(
        finish,
        out_shape=shapes,
        in_specs=[vmem] * 3,
        out_specs=(far_off,) * 3,
        scratch_shapes=[dma((PIECES + 2,))],
        compiler_params=pltpu.CompilerParams(vmem_limit_bytes=16 * 2**20),
    )(*grads)


def solution(mesh):
    return jax.shard_map(
        per_device,
        mesh=mesh,
        in_specs=(
            P("rec", "ctx", None),
            P("rec", "ctx", None),
            P("rec", None, "ctx"),
            P("rec", None, "ctx"),
            P("ctx", None),
            P("ctx", None),
            P("rec", None),
        ),
        out_specs=(P("rec", "ctx", None), P(("ctx", "rec"), None), P(("ctx", "rec"), None)),
        check_vma=False,
    )
```

```python
import math

import jax
import jax.numpy as jnp
from jax import lax
from jax.experimental import pallas as pl
from jax.experimental.pallas import tpu as pltpu
from jax.sharding import PartitionSpec as P

HD = 128
MAXSPAN = 4
HEADS = 16
BACK = MAXSPAN - 1
MESH = pl.DeviceIdType.MESH
FAR = 1e30
PIECES = 4


def kernel(
    q_hbm, g_hbm, sums_hbm, delta_hbm, k_hbm, v_hbm, ids_hbm,
    dq_ref, dk_ref, dv_ref,
    q_buf, g_buf, sums_ref, delta_ref, ids_ref, kv, key_t, ds_buf, acc, part, mate, side_land,
    direct_land, skip_land, total, r_send, r_land,
    load_sem, own_sem, small_sem, hop_sem, near_sem, far_sem, pass_sem, mate_sem, side_sem,
    direct_sem, skip_sem, rec_sem, ready_sem,
):
    peers = lax.axis_size("ctx")
    recs = lax.axis_size("rec")
    mine = lax.axis_index("ctx")
    rec = lax.axis_index("rec")
    rows = q_buf.shape[0]
    key_heads = kv.shape[0]
    group = q_buf.shape[1] // (key_heads * HD)
    chunks = group // HEADS
    wide = HEADS * HD
    scale = HD ** (-0.5)
    fold = scale * math.log2(math.e)
    share = rows // recs
    last = key_heads - 1
    odd = lax.rem(mine, 2)
    even = 1 - odd
    partner = mine + even - odd
    first_k = 1 + 2 * odd
    side_k = 3 - 2 * odd

    def slot(k):
        if isinstance(k, int):
            return pl.ds(k * rows, rows)
        return pl.ds(pl.multiple_of(k * rows, rows), rows)

    def own_copy(g, which):
        source = (k_hbm, v_hbm)[which]
        return pltpu.make_async_copy(
            source.at[:, pl.ds(g * HD, HD)], kv.at[g, which, pl.ds(0, rows), :], own_sem.at[g, which]
        )

    def lanes(g, c):
        return pl.ds(pl.multiple_of((g * chunks + c) * wide, wide), wide)

    def load(g, c, which):
        source, target = ((q_hbm, q_buf), (g_hbm, g_buf))[which]
        return pltpu.make_async_copy(
            source.at[0, :, lanes(g, c)], target.at[:, lanes(g, c)], load_sem.at[g, c, which]
        )

    def remote(source, target, sems, device):
        return pltpu.make_async_remote_copy(
            src_ref=source, dst_ref=target, send_sem=sems.at[0], recv_sem=sems.at[1],
            device_id=device, device_id_type=MESH,
        )

    def ship(g, k, sems, device):
        return [remote(kv.at[g, :, slot(0), :], kv.at[g, :, slot(k), :], sems.at[g], {"ctx": device})]

    def hop(g):
        return ship(g, 2, hop_sem, lax.rem(mine + 2, peers))

    def near(g):
        return ship(g, 1, near_sem, partner)

    def far(g):
        return ship(g, 3, far_sem, lax.rem(mine + 3, peers))

    def hand(g):
        return remote(kv.at[g, :, slot(2), :], kv.at[g, :, slot(side_k), :], pass_sem.at[g], {"ctx": partner})

    def mate_copy(g):
        return remote(part.at[g, first_k - 1], mate.at[g], mate_sem.at[g], {"ctx": partner})

    def side_copy(g):
        return remote(part.at[g, 0], side_land.at[g], side_sem.at[g], {"ctx": partner})

    def shares(ref, target):
        return ref.at[:, pl.ds(pl.multiple_of(target * share, share), share), :]

    def scatter(g, k, land, sems, target, slot_there):
        return pltpu.make_async_remote_copy(
            src_ref=shares(part.at[g, k - 1], target), dst_ref=land.at[g, slot_there],
            send_sem=sems.at[g, target, 0], recv_sem=sems.at[g, slot_there, 1],
            device_id={"ctx": lax.rem(mine - k + peers, peers), "rec": target}, device_id_type=MESH,
        )

    def direct_copy(g, target):
        return scatter(g, 2, direct_land, direct_sem, target, rec)

    def skip_copy(g, target):
        return scatter(g, 3, skip_land, skip_sem, target, rec)

    def direct_from(g, source):
        return scatter(g, 2, direct_land, direct_sem, source, source)

    def skip_from(g, source):
        return scatter(g, 3, skip_land, skip_sem, source, source)

    def rec_copy(g, j):
        target = lax.rem(rec + j, recs)
        return remote(shares(r_send.at[g], target), r_land.at[g, j - 1], rec_sem.at[g, j - 1], {"rec": target})

    barrier = pltpu.get_barrier_semaphore()
    third = mine + 3 * odd - 3 * even
    greeted = jnp.int32(recs - 1)
    for other in (partner, mine + 2, mine - 2, third):
        there = (other >= 0) & (other < peers)
        greeted = greeted + jnp.where(there, 1, 0)

        @pl.when(there)
        def _():
            pl.semaphore_signal(barrier, inc=1, device_id={"ctx": other}, device_id_type=MESH)
    for j in range(1, recs):
        pl.semaphore_signal(
            barrier, inc=1, device_id={"rec": lax.rem(rec + j, recs)}, device_id_type=MESH
        )

    def begin(copies):
        for copy in copies:
            copy.start()

    def landed(copies):
        for copy in copies:
            copy.wait_recv()

    def sent(copies):
        for copy in copies:
            copy.wait_send()

    for g in range(key_heads):
        for which in range(2):
            own_copy(g, which).start()
    small = [
        pltpu.make_async_copy(source, target, small_sem.at[i])
        for i, (source, target) in enumerate(
            ((sums_hbm, sums_ref), (delta_hbm, delta_ref), (ids_hbm, ids_ref))
        )
    ]
    for copy in small:
        copy.start()
    for g in range(key_heads):
        for c in range(chunks):
            for which in range(2):
                load(g, c, which).start()

    for k in range(1, MAXSPAN):
        @pl.when(mine < k)
        def _():
            kv[:, :, pl.ds(k * rows, rows), :] = jnp.zeros((key_heads, 2, rows, HD), kv.dtype)

    @pl.when(mine < 2)
    def _():
        mate[...] = jnp.zeros_like(mate)

    @pl.when(mine + 2 >= peers)
    def _():
        direct_land[...] = jnp.zeros_like(direct_land)

    @pl.when((even == 1) | (mine + 3 >= peers))
    def _():
        skip_land[...] = jnp.zeros_like(skip_land)

    acc[...] = jnp.zeros_like(acc)
    pl.semaphore_wait(barrier, greeted)
    for j in range(1, recs):
        pl.semaphore_signal(
            ready_sem, inc=1, device_id={"rec": lax.rem(rec + j, recs)}, device_id_type=MESH
        )

    for g in range(key_heads):
        for which in range(2):
            own_copy(g, which).wait()

        @pl.when(mine + 2 < peers)
        def _():
            begin(hop(g))

        @pl.when(even == 1)
        def _():
            begin(near(g))

    for copy in small:
        copy.wait()
    here = ids_ref[0, mine]

    def away(k):
        if isinstance(k, int) and k == 0:
            return jnp.float32(0.0)
        same = (ids_ref[0, jnp.maximum(mine - k, 0)] == here) & (mine >= k)
        return jnp.where(same, 0.0, FAR).astype(jnp.float32)

    def heads_down(ref, g, c):
        first = (g * chunks + c) * HEADS
        return jnp.concatenate(
            [ref[:, pl.ds(pl.multiple_of((first + i) * HD, HD), HD)] for i in range(HEADS)], axis=0
        )

    def heads_along(ref, g, c):
        first = (g * chunks + c) * HEADS
        return jnp.concatenate([ref[0, pl.ds(first + i, 1), :] for i in range(HEADS)], axis=1)

    inner = (((1,), (1,)), ((), ()))

    def sweep(g, k):
        at = slot(k)
        own = isinstance(k, int) and k == 0
        shift = away(k)

        @pl.loop(0, chunks)
        def _(c):
            if own:
                for which in range(2):
                    load(g, c, which).wait()
            query = heads_down(q_buf, g, c)
            grad = heads_down(g_buf, g, c)
            sums = heads_along(sums_ref, g, c) * math.log2(math.e) + shift
            delta = heads_along(delta_ref, g, c)
            scores = lax.dot_general(
                kv[g, 0, at, :], query, inner, preferred_element_type=jnp.float32
            )
            dprobs = lax.dot_general(
                kv[g, 1, at, :], grad, inner, preferred_element_type=jnp.float32
            )
            probs = jnp.exp2(scores * fold - sums)
            if own:
                u = lax.broadcasted_iota(jnp.int32, (rows, wide), 0)
                t = lax.broadcasted_iota(jnp.int32, (rows, wide), 1) & (rows - 1)
                probs = jnp.where(u <= t, probs, 0.0)
            ds = (probs * (dprobs - delta)).astype(jnp.bfloat16)
            probs = probs.astype(jnp.bfloat16)
            ds_buf[at, lanes(g, c)] = ds
            acc[g, 0, at, :] += jnp.dot(ds, query, preferred_element_type=jnp.float32)
            acc[g, 1, at, :] += jnp.dot(probs, grad, preferred_element_type=jnp.float32)

        key_t[g, :, slot(k)] = kv[g, 0, at, :].T

    def query_side(g):
        @pl.loop(0, chunks)
        def _(c):
            dq = jnp.dot(
                key_t[g], ds_buf[:, lanes(g, c)], preferred_element_type=jnp.float32
            ) * scale
            for i in range(HEADS):
                at = pl.ds(pl.multiple_of(((g * chunks + c) * HEADS + i) * HD, HD), HD)
                dq_ref[0, :, at] = dq[:, i * rows:(i + 1) * rows].T.astype(dq_ref.dtype)

    def keep(g, k):
        part[g, k - 1] = acc[g, :, slot(k), :].astype(part.dtype)

    def arrive(g):
        @pl.when(mine >= 2)
        def _():
            landed(hop(g))
            hand(g).start()

    def combine(g):
        @pl.when(mine >= 2)
        def _():
            mate_copy(g).wait_recv()
        whole = acc[g, :, slot(2), :] + mate[g].astype(jnp.float32)
        part[g, 1] = whole.astype(part.dtype)

        @pl.when(mine >= 2)
        def _():
            for j in range(recs):
                direct_copy(g, j).start()

    def send_mate(g):
        keep(g, first_k)

        @pl.when(mine >= 2)
        def _():
            mate_copy(g).start()

    def send_skip(g):
        keep(g, 3)

        @pl.when(mine >= 3)
        def _():
            for j in range(recs):
                skip_copy(g, j).start()

    def wait_far(g):
        @pl.when(mine >= 3)
        def _():
            landed(far(g))

    def wait_hand(g):
        @pl.when(mine >= 2)
        def _():
            hand(g).wait_recv()

    def across(g, with_side):
        whole = acc[g, :, 0:rows, :]
        if with_side:
            side_copy(g).wait_recv()
            whole = whole + side_land[g].astype(jnp.float32)
        total[g] = whole
        r_send[g] = whole.astype(r_send.dtype)
        for j in range(1, recs):
            rec_copy(g, j).start()

    def close(g):
        whole = total[g, :, pl.ds(pl.multiple_of(rec * share, share), share), :]
        for j in range(1, recs):
            rec_copy(g, j).wait_recv()
            whole = whole + r_land[g, j - 1].astype(jnp.float32)

        @pl.when(mine + 2 < peers)
        def _():
            for j in range(recs):
                direct_from(g, j).wait_recv()

        @pl.when((odd == 1) & (mine + 3 < peers))
        def _():
            for j in range(recs):
                skip_from(g, j).wait_recv()
        for j in range(recs):
            whole = whole + direct_land[g, j].astype(jnp.float32) + skip_land[g, j].astype(jnp.float32)
        dk_ref[:, g * HD:(g + 1) * HD] = (whole[0] * scale).astype(dk_ref.dtype)
        dv_ref[:, g * HD:(g + 1) * HD] = whole[1].astype(dv_ref.dtype)

    for g in range(key_heads):
        sweep(g, 0)

    @pl.when(odd == 1)
    def _():
        for g in range(key_heads):
            across(g, False)
        for g in range(key_heads):
            landed(near(g))
            sweep(g, 1)
            keep(g, 1)
            side_copy(g).start()
            if g == 0:
                @pl.when(mine + 3 < peers)
                def _():
                    for h in range(key_heads):
                        begin(far(h))

    arrive(0)
    sweep(0, 2)
    for g in range(1, key_heads):
        arrive(g)
    wait_hand(0)
    sweep(0, first_k)
    send_mate(0)
    pl.semaphore_wait(ready_sem, recs - 1)

    @pl.when(even == 1)
    def _():
        for g in range(key_heads):
            across(g, True)
        for g in range(key_heads):
            if g > 0:
                wait_hand(g)
                sweep(g, 1)
                send_mate(g)
                combine(g - 1)
            wait_far(g)
            sweep(g, 3)
            send_skip(g)
        sweep(last, 2)

    @pl.when(odd == 1)
    def _():
        for g in range(1, key_heads):
            sweep(g, 2)
            combine(g - 1)
            wait_hand(g)
            sweep(g, 3)
            send_mate(g)
    combine(last)
    for g in range(key_heads):
        query_side(g)
    for g in range(key_heads):
        close(g)
    for g in range(key_heads):
        @pl.when(mine + 2 < peers)
        def _():
            sent(hop(g))

        @pl.when(even == 1)
        def _():
            sent(near(g))

        @pl.when((odd == 1) & (mine + 3 < peers))
        def _():
            sent(far(g))

        @pl.when(mine >= 2)
        def _():
            hand(g).wait_send()
            mate_copy(g).wait_send()
            for j in range(recs):
                direct_copy(g, j).wait_send()

        @pl.when(odd == 1)
        def _():
            side_copy(g).wait_send()

        @pl.when((even == 1) & (mine >= 3))
        def _():
            for j in range(recs):
                skip_copy(g, j).wait_send()
        for j in range(1, recs):
            rec_copy(g, j).wait_send()


def finish(dq_in, dk_in, dv_in, dq_out, dk_out, dv_out, out):
    depth = dq_in.shape[1] // PIECES
    pairs = [
        (dq_in.at[0, pl.ds(i * depth, depth), :], dq_out.at[0, pl.ds(i * depth, depth), :])
        for i in range(PIECES)
    ] + [(dk_in, dk_out), (dv_in, dv_out)]
    outs = [pltpu.make_async_copy(p[0], p[1], out.at[i]) for i, p in enumerate(pairs)]
    for copy in outs:
        copy.start()
    for copy in outs:
        copy.wait()


def per_device(queries, out_grads, log_sums, deltas, keys, values, doc_ids):
    recs = lax.axis_size("rec")
    rows, width = queries.shape[1:]
    key_heads = keys.shape[1] // HD
    chunks = width // (key_heads * HD * HEADS)
    span = MAXSPAN * rows
    half = jnp.bfloat16
    dma = pltpu.SemaphoreType.DMA
    far_off = pl.BlockSpec(memory_space=pltpu.HBM)
    vmem = pl.BlockSpec(memory_space=pltpu.VMEM)
    small = (rows // recs, keys.shape[1])
    shapes = (
        jax.ShapeDtypeStruct(queries.shape, half),
        jax.ShapeDtypeStruct(small, half),
        jax.ShapeDtypeStruct(small, half),
    )
    pair = (key_heads, 2, rows, HD)
    grads = pl.pallas_call(
        kernel,
        out_shape=shapes,
        in_specs=[far_off] * 7,
        out_specs=(vmem, vmem, vmem),
        scratch_shapes=[
            pltpu.VMEM((rows, width), half),
            pltpu.VMEM((rows, width), half),
            pltpu.VMEM(log_sums.shape, jnp.float32),
            pltpu.VMEM(deltas.shape, jnp.float32),
            pltpu.SMEM(doc_ids.shape, jnp.int32),
            pltpu.VMEM((key_heads, 2, span, HD), half),
            pltpu.VMEM((key_heads, HD, span), half),
            pltpu.VMEM((span, width), half),
            pltpu.VMEM((key_heads, 2, span, HD), jnp.float32),
            pltpu.VMEM((key_heads, BACK, 2, rows, HD), half),
            pltpu.VMEM(pair, half),
            pltpu.VMEM(pair, half),
            pltpu.VMEM((key_heads, recs, 2, rows // recs, HD), half),
            pltpu.VMEM((key_heads, recs, 2, rows // recs, HD), half),
            pltpu.VMEM(pair, jnp.float32),
            pltpu.VMEM(pair, half),
            pltpu.VMEM((key_heads, max(recs - 1, 1), 2, rows // recs, HD), half),
            dma((key_heads, chunks, 2)),
            dma((key_heads, 2)),
            dma((3,)),
            dma((key_heads, 2)),
            dma((key_heads, 2)),
            dma((key_heads, 2)),
            dma((key_heads, 2)),
            dma((key_heads, 2)),
            dma((key_heads, 2)),
            dma((key_heads, recs, 2)),
            dma((key_heads, recs, 2)),
            dma((key_heads, max(recs - 1, 1), 2)),
            pltpu.SemaphoreType.REGULAR,
        ],
        compiler_params=pltpu.CompilerParams(
            collective_id=0, has_side_effects=True, vmem_limit_bytes=40 * 2**20
        ),
    )(*[
        pltpu.with_memory_space_constraint(x, pltpu.HBM)
        for x in (queries, out_grads, log_sums, deltas, keys, values, doc_ids)
    ])
    return pl.pallas_call(
        finish,
        out_shape=shapes,
        in_specs=[vmem] * 3,
        out_specs=(far_off,) * 3,
        scratch_shapes=[dma((PIECES + 2,))],
        compiler_params=pltpu.CompilerParams(vmem_limit_bytes=16 * 2**20),
    )(*grads)


def solution(mesh):
    return jax.shard_map(
        per_device,
        mesh=mesh,
        in_specs=(
            P("rec", "ctx", None),
            P("rec", "ctx", None),
            P("rec", None, "ctx"),
            P("rec", None, "ctx"),
            P("ctx", None),
            P("ctx", None),
            P("rec", None),
        ),
        out_specs=(P("rec", "ctx", None), P(("ctx", "rec"), None), P(("ctx", "rec"), None)),
        check_vma=False,
    )
```

```python
import math

import jax
import jax.numpy as jnp
from jax import lax
from jax.experimental import pallas as pl
from jax.experimental.pallas import tpu as pltpu
from jax.sharding import PartitionSpec as P

HD = 128
MAXSPAN = 4
HEADS = 16
BACK = MAXSPAN - 1
MESH = pl.DeviceIdType.MESH
FAR = 1e30
PIECES = 1


def kernel(
    q_hbm, g_hbm, sums_hbm, delta_hbm, k_hbm, v_hbm, ids_hbm,
    dq_ref, dk_ref, dv_ref,
    q_buf, g_buf, sums_ref, delta_ref, ids_ref, kv, key_t, ds_buf, acc, part, mate, side_land,
    direct_land, skip_land, total, r_send, r_land,
    load_sem, own_sem, small_sem, hop_sem, near_sem, far_sem, pass_sem, mate_sem, side_sem,
    direct_sem, skip_sem, rec_sem, ready_sem,
):
    peers = lax.axis_size("ctx")
    recs = lax.axis_size("rec")
    mine = lax.axis_index("ctx")
    rec = lax.axis_index("rec")
    rows = q_buf.shape[0]
    key_heads = kv.shape[0]
    group = q_buf.shape[1] // (key_heads * HD)
    chunks = group // HEADS
    wide = HEADS * HD
    scale = HD ** (-0.5)
    fold = scale * math.log2(math.e)
    share = rows // recs
    last = key_heads - 1
    odd = lax.rem(mine, 2)
    even = 1 - odd
    partner = mine + even - odd
    first_k = 1 + 2 * odd
    side_k = 3 - 2 * odd

    def slot(k):
        if isinstance(k, int):
            return pl.ds(k * rows, rows)
        return pl.ds(pl.multiple_of(k * rows, rows), rows)

    def own_copy(g, which):
        source = (k_hbm, v_hbm)[which]
        return pltpu.make_async_copy(
            source.at[:, pl.ds(g * HD, HD)], kv.at[g, which, pl.ds(0, rows), :], own_sem.at[g, which]
        )

    def lanes(g, c):
        return pl.ds(pl.multiple_of((g * chunks + c) * wide, wide), wide)

    def load(g, c, which):
        source, target = ((q_hbm, q_buf), (g_hbm, g_buf))[which]
        return pltpu.make_async_copy(
            source.at[0, :, lanes(g, c)], target.at[:, lanes(g, c)], load_sem.at[g, c, which]
        )

    def remote(source, target, sems, device):
        return pltpu.make_async_remote_copy(
            src_ref=source, dst_ref=target, send_sem=sems.at[0], recv_sem=sems.at[1],
            device_id=device, device_id_type=MESH,
        )

    def ship(g, k, sems, device):
        return [remote(kv.at[g, :, slot(0), :], kv.at[g, :, slot(k), :], sems.at[g], {"ctx": device})]

    def hop(g):
        return ship(g, 2, hop_sem, lax.rem(mine + 2, peers))

    def near(g):
        return ship(g, 1, near_sem, partner)

    def far(g):
        return ship(g, 3, far_sem, lax.rem(mine + 3, peers))

    def hand(g):
        return remote(kv.at[g, :, slot(2), :], kv.at[g, :, slot(side_k), :], pass_sem.at[g], {"ctx": partner})

    def mate_copy(g):
        return remote(part.at[g, first_k - 1], mate.at[g], mate_sem.at[g], {"ctx": partner})

    def side_copy(g):
        return remote(part.at[g, 0], side_land.at[g], side_sem.at[g], {"ctx": partner})

    def shares(ref, target):
        return ref.at[:, pl.ds(pl.multiple_of(target * share, share), share), :]

    def scatter(g, k, land, sems, target, slot_there):
        return pltpu.make_async_remote_copy(
            src_ref=shares(part.at[g, k - 1], target), dst_ref=land.at[g, slot_there],
            send_sem=sems.at[g, target, 0], recv_sem=sems.at[g, slot_there, 1],
            device_id={"ctx": lax.rem(mine - k + peers, peers), "rec": target}, device_id_type=MESH,
        )

    def direct_copy(g, target):
        return scatter(g, 2, direct_land, direct_sem, target, rec)

    def skip_copy(g, target):
        return scatter(g, 3, skip_land, skip_sem, target, rec)

    def direct_from(g, source):
        return scatter(g, 2, direct_land, direct_sem, source, source)

    def skip_from(g, source):
        return scatter(g, 3, skip_land, skip_sem, source, source)

    def rec_copy(g, j):
        target = lax.rem(rec + j, recs)
        return remote(shares(r_send.at[g], target), r_land.at[g, j - 1], rec_sem.at[g, j - 1], {"rec": target})

    barrier = pltpu.get_barrier_semaphore()
    third = mine + 3 * odd - 3 * even
    greeted = jnp.int32(recs - 1)
    for other in (partner, mine + 2, mine - 2, third):
        there = (other >= 0) & (other < peers)
        greeted = greeted + jnp.where(there, 1, 0)

        @pl.when(there)
        def _():
            pl.semaphore_signal(barrier, inc=1, device_id={"ctx": other}, device_id_type=MESH)
    for j in range(1, recs):
        pl.semaphore_signal(
            barrier, inc=1, device_id={"rec": lax.rem(rec + j, recs)}, device_id_type=MESH
        )

    def begin(copies):
        for copy in copies:
            copy.start()

    def landed(copies):
        for copy in copies:
            copy.wait_recv()

    def sent(copies):
        for copy in copies:
            copy.wait_send()

    for g in range(key_heads):
        for which in range(2):
            own_copy(g, which).start()
    small = [
        pltpu.make_async_copy(source, target, small_sem.at[i])
        for i, (source, target) in enumerate(
            ((sums_hbm, sums_ref), (delta_hbm, delta_ref), (ids_hbm, ids_ref))
        )
    ]
    for copy in small:
        copy.start()
    for g in range(key_heads):
        for c in range(chunks):
            for which in range(2):
                load(g, c, which).start()

    for k in range(1, MAXSPAN):
        @pl.when(mine < k)
        def _():
            kv[:, :, pl.ds(k * rows, rows), :] = jnp.zeros((key_heads, 2, rows, HD), kv.dtype)

    @pl.when(mine < 2)
    def _():
        mate[...] = jnp.zeros_like(mate)

    @pl.when(mine + 2 >= peers)
    def _():
        direct_land[...] = jnp.zeros_like(direct_land)

    @pl.when((even == 1) | (mine + 3 >= peers))
    def _():
        skip_land[...] = jnp.zeros_like(skip_land)

    acc[...] = jnp.zeros_like(acc)
    pl.semaphore_wait(barrier, greeted)
    for j in range(1, recs):
        pl.semaphore_signal(
            ready_sem, inc=1, device_id={"rec": lax.rem(rec + j, recs)}, device_id_type=MESH
        )

    for g in range(key_heads):
        for which in range(2):
            own_copy(g, which).wait()

        @pl.when(mine + 2 < peers)
        def _():
            begin(hop(g))

        @pl.when(even == 1)
        def _():
            begin(near(g))

    for copy in small:
        copy.wait()
    here = ids_ref[0, mine]

    def away(k):
        if isinstance(k, int) and k == 0:
            return jnp.float32(0.0)
        same = (ids_ref[0, jnp.maximum(mine - k, 0)] == here) & (mine >= k)
        return jnp.where(same, 0.0, FAR).astype(jnp.float32)

    def heads_down(ref, g, c):
        first = (g * chunks + c) * HEADS
        return jnp.concatenate(
            [ref[:, pl.ds(pl.multiple_of((first + i) * HD, HD), HD)] for i in range(HEADS)], axis=0
        )

    def heads_along(ref, g, c):
        first = (g * chunks + c) * HEADS
        return jnp.concatenate([ref[0, pl.ds(first + i, 1), :] for i in range(HEADS)], axis=1)

    inner = (((1,), (1,)), ((), ()))

    def sweep(g, k):
        at = slot(k)
        own = isinstance(k, int) and k == 0
        shift = away(k)

        @pl.loop(0, chunks)
        def _(c):
            if own:
                for which in range(2):
                    load(g, c, which).wait()
            query = heads_down(q_buf, g, c)
            grad = heads_down(g_buf, g, c)
            sums = heads_along(sums_ref, g, c) * math.log2(math.e) + shift
            delta = heads_along(delta_ref, g, c)
            scores = lax.dot_general(
                kv[g, 0, at, :], query, inner, preferred_element_type=jnp.float32
            )
            dprobs = lax.dot_general(
                kv[g, 1, at, :], grad, inner, preferred_element_type=jnp.float32
            )
            probs = jnp.exp2(scores * fold - sums)
            if own:
                u = lax.broadcasted_iota(jnp.int32, (rows, wide), 0)
                t = lax.broadcasted_iota(jnp.int32, (rows, wide), 1) & (rows - 1)
                probs = jnp.where(u <= t, probs, 0.0)
            ds = (probs * (dprobs - delta)).astype(jnp.bfloat16)
            probs = probs.astype(jnp.bfloat16)
            ds_buf[at, lanes(g, c)] = ds
            acc[g, 0, at, :] += jnp.dot(ds, query, preferred_element_type=jnp.float32)
            acc[g, 1, at, :] += jnp.dot(probs, grad, preferred_element_type=jnp.float32)

        key_t[g, :, slot(k)] = kv[g, 0, at, :].T

    def query_side(g):
        @pl.loop(0, chunks)
        def _(c):
            dq = jnp.dot(
                key_t[g], ds_buf[:, lanes(g, c)], preferred_element_type=jnp.float32
            ) * scale
            for i in range(HEADS):
                at = pl.ds(pl.multiple_of(((g * chunks + c) * HEADS + i) * HD, HD), HD)
                dq_ref[0, :, at] = dq[:, i * rows:(i + 1) * rows].T.astype(dq_ref.dtype)

    def keep(g, k):
        part[g, k - 1] = acc[g, :, slot(k), :].astype(part.dtype)

    def arrive(g):
        @pl.when(mine >= 2)
        def _():
            landed(hop(g))
            hand(g).start()

    def combine(g):
        @pl.when(mine >= 2)
        def _():
            mate_copy(g).wait_recv()
        whole = acc[g, :, slot(2), :] + mate[g].astype(jnp.float32)
        part[g, 1] = whole.astype(part.dtype)

        @pl.when(mine >= 2)
        def _():
            for j in range(recs):
                direct_copy(g, j).start()

    def send_mate(g):
        keep(g, first_k)

        @pl.when(mine >= 2)
        def _():
            mate_copy(g).start()

    def send_skip(g):
        keep(g, 3)

        @pl.when(mine >= 3)
        def _():
            for j in range(recs):
                skip_copy(g, j).start()

    def wait_far(g):
        @pl.when(mine >= 3)
        def _():
            landed(far(g))

    def wait_hand(g):
        @pl.when(mine >= 2)
        def _():
            hand(g).wait_recv()

    def across(g, with_side):
        whole = acc[g, :, 0:rows, :]
        if with_side:
            side_copy(g).wait_recv()
            whole = whole + side_land[g].astype(jnp.float32)
        total[g] = whole
        r_send[g] = whole.astype(r_send.dtype)
        for j in range(1, recs):
            rec_copy(g, j).start()

    def close(g):
        whole = total[g, :, pl.ds(pl.multiple_of(rec * share, share), share), :]
        for j in range(1, recs):
            rec_copy(g, j).wait_recv()
            whole = whole + r_land[g, j - 1].astype(jnp.float32)

        @pl.when(mine + 2 < peers)
        def _():
            for j in range(recs):
                direct_from(g, j).wait_recv()

        @pl.when((odd == 1) & (mine + 3 < peers))
        def _():
            for j in range(recs):
                skip_from(g, j).wait_recv()
        for j in range(recs):
            whole = whole + direct_land[g, j].astype(jnp.float32) + skip_land[g, j].astype(jnp.float32)
        dk_ref[:, g * HD:(g + 1) * HD] = (whole[0] * scale).astype(dk_ref.dtype)
        dv_ref[:, g * HD:(g + 1) * HD] = whole[1].astype(dv_ref.dtype)

    for g in range(key_heads):
        sweep(g, 0)

    @pl.when(odd == 1)
    def _():
        for g in range(key_heads):
            across(g, False)
        for g in range(key_heads):
            landed(near(g))
            sweep(g, 1)
            keep(g, 1)
            side_copy(g).start()

        @pl.when(mine + 3 < peers)
        def _():
            for h in range(key_heads):
                begin(far(h))

    arrive(0)
    sweep(0, 2)
    for g in range(1, key_heads):
        arrive(g)
    wait_hand(0)
    sweep(0, first_k)
    send_mate(0)
    pl.semaphore_wait(ready_sem, recs - 1)

    @pl.when(even == 1)
    def _():
        for g in range(key_heads):
            if g > 0:
                wait_hand(g)
                sweep(g, 1)
                send_mate(g)
                combine(g - 1)
            wait_far(g)
            sweep(g, 3)
            send_skip(g)
        sweep(last, 2)
        combine(last)
        for g in range(key_heads):
            across(g, True)

    @pl.when(odd == 1)
    def _():
        for g in range(1, key_heads):
            combine(g - 1)
            wait_hand(g)
            sweep(g, 3)
            send_mate(g)
            sweep(g, 2)
        combine(last)
    for g in range(key_heads):
        query_side(g)
    for g in range(key_heads):
        close(g)
    for g in range(key_heads):
        @pl.when(mine + 2 < peers)
        def _():
            sent(hop(g))

        @pl.when(even == 1)
        def _():
            sent(near(g))

        @pl.when((odd == 1) & (mine + 3 < peers))
        def _():
            sent(far(g))

        @pl.when(mine >= 2)
        def _():
            hand(g).wait_send()
            mate_copy(g).wait_send()
            for j in range(recs):
                direct_copy(g, j).wait_send()

        @pl.when(odd == 1)
        def _():
            side_copy(g).wait_send()

        @pl.when((even == 1) & (mine >= 3))
        def _():
            for j in range(recs):
                skip_copy(g, j).wait_send()
        for j in range(1, recs):
            rec_copy(g, j).wait_send()


def finish(dq_in, dk_in, dv_in, dq_out, dk_out, dv_out, out):
    depth = dq_in.shape[1] // PIECES
    pairs = [
        (dq_in.at[0, pl.ds(i * depth, depth), :], dq_out.at[0, pl.ds(i * depth, depth), :])
        for i in range(PIECES)
    ] + [(dk_in, dk_out), (dv_in, dv_out)]
    outs = [pltpu.make_async_copy(p[0], p[1], out.at[i]) for i, p in enumerate(pairs)]
    for copy in outs:
        copy.start()
    for copy in outs:
        copy.wait()


def per_device(queries, out_grads, log_sums, deltas, keys, values, doc_ids):
    recs = lax.axis_size("rec")
    rows, width = queries.shape[1:]
    key_heads = keys.shape[1] // HD
    chunks = width // (key_heads * HD * HEADS)
    span = MAXSPAN * rows
    half = jnp.bfloat16
    dma = pltpu.SemaphoreType.DMA
    far_off = pl.BlockSpec(memory_space=pltpu.HBM)
    vmem = pl.BlockSpec(memory_space=pltpu.VMEM)
    small = (rows // recs, keys.shape[1])
    shapes = (
        jax.ShapeDtypeStruct(queries.shape, half),
        jax.ShapeDtypeStruct(small, half),
        jax.ShapeDtypeStruct(small, half),
    )
    pair = (key_heads, 2, rows, HD)
    grads = pl.pallas_call(
        kernel,
        out_shape=shapes,
        in_specs=[far_off] * 7,
        out_specs=(vmem, vmem, vmem),
        scratch_shapes=[
            pltpu.VMEM((rows, width), half),
            pltpu.VMEM((rows, width), half),
            pltpu.VMEM(log_sums.shape, jnp.float32),
            pltpu.VMEM(deltas.shape, jnp.float32),
            pltpu.SMEM(doc_ids.shape, jnp.int32),
            pltpu.VMEM((key_heads, 2, span, HD), half),
            pltpu.VMEM((key_heads, HD, span), half),
            pltpu.VMEM((span, width), half),
            pltpu.VMEM((key_heads, 2, span, HD), jnp.float32),
            pltpu.VMEM((key_heads, BACK, 2, rows, HD), half),
            pltpu.VMEM(pair, half),
            pltpu.VMEM(pair, half),
            pltpu.VMEM((key_heads, recs, 2, rows // recs, HD), half),
            pltpu.VMEM((key_heads, recs, 2, rows // recs, HD), half),
            pltpu.VMEM(pair, jnp.float32),
            pltpu.VMEM(pair, half),
            pltpu.VMEM((key_heads, max(recs - 1, 1), 2, rows // recs, HD), half),
            dma((key_heads, chunks, 2)),
            dma((key_heads, 2)),
            dma((3,)),
            dma((key_heads, 2)),
            dma((key_heads, 2)),
            dma((key_heads, 2)),
            dma((key_heads, 2)),
            dma((key_heads, 2)),
            dma((key_heads, 2)),
            dma((key_heads, recs, 2)),
            dma((key_heads, recs, 2)),
            dma((key_heads, max(recs - 1, 1), 2)),
            pltpu.SemaphoreType.REGULAR,
        ],
        compiler_params=pltpu.CompilerParams(
            collective_id=0, has_side_effects=True, vmem_limit_bytes=40 * 2**20
        ),
    )(*[
        pltpu.with_memory_space_constraint(x, pltpu.HBM)
        for x in (queries, out_grads, log_sums, deltas, keys, values, doc_ids)
    ])
    return pl.pallas_call(
        finish,
        out_shape=shapes,
        in_specs=[vmem] * 3,
        out_specs=(far_off,) * 3,
        scratch_shapes=[dma((PIECES + 2,))],
        compiler_params=pltpu.CompilerParams(vmem_limit_bytes=16 * 2**20),
    )(*grads)


def solution(mesh):
    return jax.shard_map(
        per_device,
        mesh=mesh,
        in_specs=(
            P("rec", "ctx", None),
            P("rec", "ctx", None),
            P("rec", None, "ctx"),
            P("rec", None, "ctx"),
            P("ctx", None),
            P("ctx", None),
            P("rec", None),
        ),
        out_specs=(P("rec", "ctx", None), P(("ctx", "rec"), None), P(("ctx", "rec"), None)),
        check_vma=False,
    )
```

```python
import math

import jax
import jax.numpy as jnp
from jax import lax
from jax.experimental import pallas as pl
from jax.experimental.pallas import tpu as pltpu
from jax.sharding import PartitionSpec as P

HD = 128
MAXSPAN = 4
HEADS = 16
BACK = MAXSPAN - 1
MESH = pl.DeviceIdType.MESH
FAR = 1e30
PIECES = 1


def kernel(
    q_hbm, g_hbm, sums_hbm, delta_hbm, k_hbm, v_hbm, ids_hbm,
    dq_ref, dk_ref, dv_ref,
    q_buf, g_buf, sums_ref, delta_ref, ids_ref, kv, key_t, ds_buf, acc, part, mate, side_land,
    direct_land, skip_land, total, r_send, r_land,
    load_sem, own_sem, small_sem, hop_sem, near_sem, far_sem, pass_sem, mate_sem, side_sem,
    direct_sem, skip_sem, rec_sem, ready_sem,
):
    peers = lax.axis_size("ctx")
    recs = lax.axis_size("rec")
    mine = lax.axis_index("ctx")
    rec = lax.axis_index("rec")
    rows = q_buf.shape[0]
    key_heads = kv.shape[0]
    group = q_buf.shape[1] // (key_heads * HD)
    chunks = group // HEADS
    wide = HEADS * HD
    scale = HD ** (-0.5)
    fold = scale * math.log2(math.e)
    share = rows // recs
    last = key_heads - 1
    odd = lax.rem(mine, 2)
    even = 1 - odd
    partner = mine + even - odd
    first_k = 1 + 2 * odd
    side_k = 3 - 2 * odd

    def slot(k):
        if isinstance(k, int):
            return pl.ds(k * rows, rows)
        return pl.ds(pl.multiple_of(k * rows, rows), rows)

    def own_copy(g, which):
        source = (k_hbm, v_hbm)[which]
        return pltpu.make_async_copy(
            source.at[:, pl.ds(g * HD, HD)], kv.at[g, which, pl.ds(0, rows), :], own_sem.at[g, which]
        )

    def lanes(g, c):
        return pl.ds(pl.multiple_of((g * chunks + c) * wide, wide), wide)

    def load(g, c, which):
        source, target = ((q_hbm, q_buf), (g_hbm, g_buf))[which]
        return pltpu.make_async_copy(
            source.at[0, :, lanes(g, c)], target.at[:, lanes(g, c)], load_sem.at[g, c, which]
        )

    def remote(source, target, sems, device):
        return pltpu.make_async_remote_copy(
            src_ref=source, dst_ref=target, send_sem=sems.at[0], recv_sem=sems.at[1],
            device_id=device, device_id_type=MESH,
        )

    def ship(g, k, sems, device):
        return [remote(kv.at[g, :, slot(0), :], kv.at[g, :, slot(k), :], sems.at[g], {"ctx": device})]

    def hop(g):
        return ship(g, 2, hop_sem, lax.rem(mine + 2, peers))

    def near(g):
        return ship(g, 1, near_sem, partner)

    def far(g):
        return ship(g, 3, far_sem, lax.rem(mine + 3, peers))

    def hand(g):
        return remote(kv.at[g, :, slot(2), :], kv.at[g, :, slot(side_k), :], pass_sem.at[g], {"ctx": partner})

    def mate_copy(g):
        return remote(part.at[g, first_k - 1], mate.at[g], mate_sem.at[g], {"ctx": partner})

    def side_copy(g):
        return remote(part.at[g, 0], side_land.at[g], side_sem.at[g], {"ctx": partner})

    def split(block):
        return jnp.stack([block[:, t * share:(t + 1) * share, :] for t in range(recs)])

    def scatter(g, k, land, sems, target, slot_there):
        return pltpu.make_async_remote_copy(
            src_ref=part.at[g, k - 1, target], dst_ref=land.at[g, slot_there],
            send_sem=sems.at[g, target, 0], recv_sem=sems.at[g, slot_there, 1],
            device_id={"ctx": lax.rem(mine - k + peers, peers), "rec": target}, device_id_type=MESH,
        )

    def direct_copy(g, target):
        return scatter(g, 2, direct_land, direct_sem, target, rec)

    def skip_copy(g, target):
        return scatter(g, 3, skip_land, skip_sem, target, rec)

    def direct_from(g, source):
        return scatter(g, 2, direct_land, direct_sem, source, source)

    def skip_from(g, source):
        return scatter(g, 3, skip_land, skip_sem, source, source)

    def rec_copy(g, j):
        target = lax.rem(rec + j, recs)
        return remote(r_send.at[g, target], r_land.at[g, j - 1], rec_sem.at[g, j - 1], {"rec": target})

    barrier = pltpu.get_barrier_semaphore()
    third = mine + 3 * odd - 3 * even
    greeted = jnp.int32(recs - 1)
    for other in (partner, mine + 2, mine - 2, third):
        there = (other >= 0) & (other < peers)
        greeted = greeted + jnp.where(there, 1, 0)

        @pl.when(there)
        def _():
            pl.semaphore_signal(barrier, inc=1, device_id={"ctx": other}, device_id_type=MESH)
    for j in range(1, recs):
        pl.semaphore_signal(
            barrier, inc=1, device_id={"rec": lax.rem(rec + j, recs)}, device_id_type=MESH
        )

    def begin(copies):
        for copy in copies:
            copy.start()

    def landed(copies):
        for copy in copies:
            copy.wait_recv()

    def sent(copies):
        for copy in copies:
            copy.wait_send()

    for g in range(key_heads):
        for which in range(2):
            own_copy(g, which).start()
    small = [
        pltpu.make_async_copy(source, target, small_sem.at[i])
        for i, (source, target) in enumerate(
            ((sums_hbm, sums_ref), (delta_hbm, delta_ref), (ids_hbm, ids_ref))
        )
    ]
    for copy in small:
        copy.start()
    for g in range(key_heads):
        for c in range(chunks):
            for which in range(2):
                load(g, c, which).start()

    for k in range(1, MAXSPAN):
        @pl.when(mine < k)
        def _():
            kv[:, :, pl.ds(k * rows, rows), :] = jnp.zeros((key_heads, 2, rows, HD), kv.dtype)

    @pl.when(mine < 2)
    def _():
        mate[...] = jnp.zeros_like(mate)

    @pl.when(mine + 2 >= peers)
    def _():
        direct_land[...] = jnp.zeros_like(direct_land)

    @pl.when((even == 1) | (mine + 3 >= peers))
    def _():
        skip_land[...] = jnp.zeros_like(skip_land)

    if chunks > 1:
        acc[...] = jnp.zeros_like(acc)
    pl.semaphore_wait(barrier, greeted)
    for j in range(1, recs):
        pl.semaphore_signal(
            ready_sem, inc=1, device_id={"rec": lax.rem(rec + j, recs)}, device_id_type=MESH
        )

    for g in range(key_heads):
        for which in range(2):
            own_copy(g, which).wait()

        @pl.when(mine + 2 < peers)
        def _():
            begin(hop(g))

        @pl.when(even == 1)
        def _():
            begin(near(g))

    for copy in small:
        copy.wait()
    here = ids_ref[0, mine]

    def away(k):
        if isinstance(k, int) and k == 0:
            return jnp.float32(0.0)
        same = (ids_ref[0, jnp.maximum(mine - k, 0)] == here) & (mine >= k)
        return jnp.where(same, 0.0, FAR).astype(jnp.float32)

    def heads_down(ref, g, c):
        first = (g * chunks + c) * HEADS
        return jnp.concatenate(
            [ref[:, pl.ds(pl.multiple_of((first + i) * HD, HD), HD)] for i in range(HEADS)], axis=0
        )

    def heads_along(ref, g, c):
        first = (g * chunks + c) * HEADS
        return jnp.concatenate([ref[0, pl.ds(first + i, 1), :] for i in range(HEADS)], axis=1)

    inner = (((1,), (1,)), ((), ()))

    def sweep(g, k):
        at = slot(k)
        own = isinstance(k, int) and k == 0
        shift = away(k)

        @pl.loop(0, chunks)
        def _(c):
            if own:
                for which in range(2):
                    load(g, c, which).wait()
            query = heads_down(q_buf, g, c)
            grad = heads_down(g_buf, g, c)
            sums = heads_along(sums_ref, g, c) * math.log2(math.e) + shift
            delta = heads_along(delta_ref, g, c)
            scores = lax.dot_general(
                kv[g, 0, at, :], query, inner, preferred_element_type=jnp.float32
            )
            dprobs = lax.dot_general(
                kv[g, 1, at, :], grad, inner, preferred_element_type=jnp.float32
            )
            probs = jnp.exp2(scores * fold - sums)
            if own:
                u = lax.broadcasted_iota(jnp.int32, (rows, wide), 0)
                t = lax.broadcasted_iota(jnp.int32, (rows, wide), 1) & (rows - 1)
                probs = jnp.where(u <= t, probs, 0.0)
            ds = (probs * (dprobs - delta)).astype(jnp.bfloat16)
            probs = probs.astype(jnp.bfloat16)
            ds_buf[at, lanes(g, c)] = ds
            key_part = jnp.dot(ds, query, preferred_element_type=jnp.float32)
            value_part = jnp.dot(probs, grad, preferred_element_type=jnp.float32)
            if chunks > 1:
                key_part = key_part + acc[g, 0, at, :]
                value_part = value_part + acc[g, 1, at, :]
            acc[g, 0, at, :] = key_part
            acc[g, 1, at, :] = value_part

        key_t[g, :, slot(k)] = kv[g, 0, at, :].T

    def query_side(g):
        @pl.loop(0, chunks)
        def _(c):
            dq = jnp.dot(
                key_t[g], ds_buf[:, lanes(g, c)], preferred_element_type=jnp.float32
            ) * scale
            for i in range(HEADS):
                at = pl.ds(pl.multiple_of(((g * chunks + c) * HEADS + i) * HD, HD), HD)
                dq_ref[0, :, at] = dq[:, i * rows:(i + 1) * rows].T.astype(dq_ref.dtype)

    def keep(g, k):
        part[g, k - 1] = split(acc[g, :, slot(k), :]).astype(part.dtype)

    def arrive(g):
        @pl.when(mine >= 2)
        def _():
            landed(hop(g))
            hand(g).start()

    def combine(g):
        @pl.when(mine >= 2)
        def _():
            mate_copy(g).wait_recv()
        whole = split(acc[g, :, slot(2), :]) + mate[g].astype(jnp.float32)
        part[g, 1] = whole.astype(part.dtype)

        @pl.when(mine >= 2)
        def _():
            for j in range(recs):
                direct_copy(g, j).start()

    def send_mate(g):
        keep(g, first_k)

        @pl.when(mine >= 2)
        def _():
            mate_copy(g).start()

    def send_skip(g):
        keep(g, 3)

        @pl.when(mine >= 3)
        def _():
            for j in range(recs):
                skip_copy(g, j).start()

    def wait_far(g):
        @pl.when(mine >= 3)
        def _():
            landed(far(g))

    def wait_hand(g):
        @pl.when(mine >= 2)
        def _():
            hand(g).wait_recv()

    def across(g, with_side):
        whole = split(acc[g, :, 0:rows, :])
        if with_side:
            side_copy(g).wait_recv()
            whole = whole + side_land[g].astype(jnp.float32)
        total[g] = whole
        r_send[g] = whole.astype(r_send.dtype)
        for j in range(1, recs):
            rec_copy(g, j).start()

    def close(g):
        whole = total[g, rec]
        for j in range(1, recs):
            rec_copy(g, j).wait_recv()
            whole = whole + r_land[g, j - 1].astype(jnp.float32)

        @pl.when(mine + 2 < peers)
        def _():
            for j in range(recs):
                direct_from(g, j).wait_recv()

        @pl.when((odd == 1) & (mine + 3 < peers))
        def _():
            for j in range(recs):
                skip_from(g, j).wait_recv()
        for j in range(recs):
            whole = whole + direct_land[g, j].astype(jnp.float32) + skip_land[g, j].astype(jnp.float32)
        dk_ref[:, g * HD:(g + 1) * HD] = (whole[0] * scale).astype(dk_ref.dtype)
        dv_ref[:, g * HD:(g + 1) * HD] = whole[1].astype(dv_ref.dtype)

    for g in range(key_heads):
        sweep(g, 0)

    @pl.when(odd == 1)
    def _():
        for g in range(key_heads):
            across(g, False)
        for g in range(key_heads):
            landed(near(g))
            sweep(g, 1)
            keep(g, 1)
            side_copy(g).start()

        @pl.when(mine + 3 < peers)
        def _():
            for h in range(key_heads):
                begin(far(h))

    arrive(0)
    sweep(0, 2)
    for g in range(1, key_heads):
        arrive(g)
    wait_hand(0)
    sweep(0, first_k)
    send_mate(0)
    pl.semaphore_wait(ready_sem, recs - 1)

    @pl.when(even == 1)
    def _():
        for g in range(key_heads):
            if g > 0:
                wait_hand(g)
                sweep(g, 1)
                send_mate(g)
                combine(g - 1)
            wait_far(g)
            sweep(g, 3)
            send_skip(g)
        sweep(last, 2)
        combine(last)
        for g in range(key_heads):
            across(g, True)

    @pl.when(odd == 1)
    def _():
        for g in range(1, key_heads):
            combine(g - 1)
            wait_hand(g)
            sweep(g, 3)
            send_mate(g)
            sweep(g, 2)
        combine(last)
    for g in range(key_heads):
        query_side(g)
    for g in range(key_heads):
        close(g)
    for g in range(key_heads):
        @pl.when(mine + 2 < peers)
        def _():
            sent(hop(g))

        @pl.when(even == 1)
        def _():
            sent(near(g))

        @pl.when((odd == 1) & (mine + 3 < peers))
        def _():
            sent(far(g))

        @pl.when(mine >= 2)
        def _():
            hand(g).wait_send()
            mate_copy(g).wait_send()
            for j in range(recs):
                direct_copy(g, j).wait_send()

        @pl.when(odd == 1)
        def _():
            side_copy(g).wait_send()

        @pl.when((even == 1) & (mine >= 3))
        def _():
            for j in range(recs):
                skip_copy(g, j).wait_send()
        for j in range(1, recs):
            rec_copy(g, j).wait_send()


def finish(dq_in, dk_in, dv_in, dq_out, dk_out, dv_out, out):
    depth = dq_in.shape[1] // PIECES
    pairs = [
        (dq_in.at[0, pl.ds(i * depth, depth), :], dq_out.at[0, pl.ds(i * depth, depth), :])
        for i in range(PIECES)
    ] + [(dk_in, dk_out), (dv_in, dv_out)]
    outs = [pltpu.make_async_copy(p[0], p[1], out.at[i]) for i, p in enumerate(pairs)]
    for copy in outs:
        copy.start()
    for copy in outs:
        copy.wait()


def per_device(queries, out_grads, log_sums, deltas, keys, values, doc_ids):
    recs = lax.axis_size("rec")
    rows, width = queries.shape[1:]
    key_heads = keys.shape[1] // HD
    chunks = width // (key_heads * HD * HEADS)
    span = MAXSPAN * rows
    half = jnp.bfloat16
    dma = pltpu.SemaphoreType.DMA
    far_off = pl.BlockSpec(memory_space=pltpu.HBM)
    vmem = pl.BlockSpec(memory_space=pltpu.VMEM)
    small = (rows // recs, keys.shape[1])
    shapes = (
        jax.ShapeDtypeStruct(queries.shape, half),
        jax.ShapeDtypeStruct(small, half),
        jax.ShapeDtypeStruct(small, half),
    )
    pair = (key_heads, recs, 2, rows // recs, HD)
    grads = pl.pallas_call(
        kernel,
        out_shape=shapes,
        in_specs=[far_off] * 7,
        out_specs=(vmem, vmem, vmem),
        scratch_shapes=[
            pltpu.VMEM((rows, width), half),
            pltpu.VMEM((rows, width), half),
            pltpu.VMEM(log_sums.shape, jnp.float32),
            pltpu.VMEM(deltas.shape, jnp.float32),
            pltpu.SMEM(doc_ids.shape, jnp.int32),
            pltpu.VMEM((key_heads, 2, span, HD), half),
            pltpu.VMEM((key_heads, HD, span), half),
            pltpu.VMEM((span, width), half),
            pltpu.VMEM((key_heads, 2, span, HD), jnp.float32),
            pltpu.VMEM((key_heads, BACK) + pair[1:], half),
            pltpu.VMEM(pair, half),
            pltpu.VMEM(pair, half),
            pltpu.VMEM((key_heads, recs, 2, rows // recs, HD), half),
            pltpu.VMEM((key_heads, recs, 2, rows // recs, HD), half),
            pltpu.VMEM(pair, jnp.float32),
            pltpu.VMEM(pair, half),
            pltpu.VMEM((key_heads, max(recs - 1, 1), 2, rows // recs, HD), half),
            dma((key_heads, chunks, 2)),
            dma((key_heads, 2)),
            dma((3,)),
            dma((key_heads, 2)),
            dma((key_heads, 2)),
            dma((key_heads, 2)),
            dma((key_heads, 2)),
            dma((key_heads, 2)),
            dma((key_heads, 2)),
            dma((key_heads, recs, 2)),
            dma((key_heads, recs, 2)),
            dma((key_heads, max(recs - 1, 1), 2)),
            pltpu.SemaphoreType.REGULAR,
        ],
        compiler_params=pltpu.CompilerParams(
            collective_id=0, has_side_effects=True, vmem_limit_bytes=40 * 2**20
        ),
    )(*[
        pltpu.with_memory_space_constraint(x, pltpu.HBM)
        for x in (queries, out_grads, log_sums, deltas, keys, values, doc_ids)
    ])
    return pl.pallas_call(
        finish,
        out_shape=shapes,
        in_specs=[vmem] * 3,
        out_specs=(far_off,) * 3,
        scratch_shapes=[dma((PIECES + 2,))],
        compiler_params=pltpu.CompilerParams(vmem_limit_bytes=16 * 2**20),
    )(*grads)


def solution(mesh):
    return jax.shard_map(
        per_device,
        mesh=mesh,
        in_specs=(
            P("rec", "ctx", None),
            P("rec", "ctx", None),
            P("rec", None, "ctx"),
            P("rec", None, "ctx"),
            P("ctx", None),
            P("ctx", None),
            P("rec", None),
        ),
        out_specs=(P("rec", "ctx", None), P(("ctx", "rec"), None), P(("ctx", "rec"), None)),
        check_vma=False,
    )
```
